32 devices in a mesh: dp: 1 (over z), tp: 4 (over y), cp: 8 (over x, core).
Axes of the slice: x: 4, y: 4, z: 1, core: 2. Of those that a mesh axis runs over, the one named last changes fastest.
The devices are a block of a 4x4x8 slice.
Arguments:
- hidden: bfloat16 [24, 768, 768], P('dp', 'cp')
- tokens: int32 [24, 768], P('dp', 'cp')
- emb_table: bfloat16 [50304, 768], P('tp')
- out_table: bfloat16 [50304, 768], P('tp')
- w_proj: bfloat16 [768, 1536], replicated
- gain_h: float32 [768], replicated
- gain_e: float32 [768], replicated
- gain_f: float32 [768], replicated
Outputs:
- output 1: float32 [1], P('dp')
- output 2: bfloat16 [24, 768, 768], P('dp', 'cp')
- output 3: float32 [768, 1536], P('dp')
- output 4: float32 [50304, 768], P(('dp', 'tp'))
- output 5: float32 [50304, 768], P(('dp', 'tp'))
- output 6: float32 [768], P('dp')
- output 7: float32 [768], P('dp')
- output 8: float32 [768], P('dp')
All inputs are finite; a program needn't handle non-finite values.
Results may differ from the reference program's by a relative error of at most 0.001.
Values sent between devices are 32-bit elements.
A program may use at most 768 MiB of HBM per device.

```python
import math
import jax
import jax.numpy as jnp
from jax import lax

BATCH_ROWS = 24
SEQ_LEN = 768
MODEL_DIM = 768
VOCAB_SIZE = 50304
MTP_WEIGHT = 0.3
NORM_EPS = 1e-6
ROW_BLOCK = math.gcd(BATCH_ROWS * SEQ_LEN, 512)


def rms_norm(values, gain):
    scale = lax.rsqrt(jnp.mean(values * values, axis=-1, keepdims=True) + NORM_EPS)
    return values * scale * gain


def draw_ids(key):
    key_level, key_pick = jax.random.split(key)
    level = jax.random.randint(key_level, (BATCH_ROWS, SEQ_LEN), 0, 8)
    upper = jnp.right_shift(jnp.full((BATCH_ROWS, SEQ_LEN), VOCAB_SIZE, jnp.int32), level)
    tok_ids = jax.random.randint(key_pick, (BATCH_ROWS, SEQ_LEN), 0, upper)
    return tok_ids.at[0, 1].set(VOCAB_SIZE - 1)


def setup_inputs(seed: int = 0, part: int = 0) -> dict:
    root_key = jax.random.key(seed)
    key_list = jax.random.split(root_key, 8)
    part_key = jax.random.fold_in(key_list[0], part)
    key_hidden, key_tokens = jax.random.split(part_key)
    hidden = jax.random.normal(key_hidden, (BATCH_ROWS, SEQ_LEN, MODEL_DIM), jnp.float32)
    emb_table = jax.random.normal(key_list[1], (VOCAB_SIZE, MODEL_DIM), jnp.float32)
    out_table = jax.random.normal(key_list[2], (VOCAB_SIZE, MODEL_DIM), jnp.float32) * (1.5 * MODEL_DIM ** -0.5)
    w_proj = jax.random.normal(key_list[3], (MODEL_DIM, 2 * MODEL_DIM), jnp.float32) * (2 * MODEL_DIM) ** -0.5
    gain_h = 1.0 + 0.25 * jax.random.normal(key_list[4], (MODEL_DIM,), jnp.float32)
    gain_e = 1.0 + 0.25 * jax.random.normal(key_list[5], (MODEL_DIM,), jnp.float32)
    gain_f = 1.0 + 0.25 * jax.random.normal(key_list[6], (MODEL_DIM,), jnp.float32)
    return {
        "hidden": hidden.astype(jnp.bfloat16),
        "tokens": draw_ids(key_tokens),
        "emb_table": emb_table.astype(jnp.bfloat16),
        "out_table": out_table.astype(jnp.bfloat16),
        "w_proj": w_proj.astype(jnp.bfloat16),
        "gain_h": gain_h,
        "gain_e": gain_e,
        "gain_f": gain_f,
    }


def reference(hidden, tokens, emb_table, out_table, w_proj, gain_h, gain_e, gain_f):
    n_blocks = (BATCH_ROWS * SEQ_LEN) // ROW_BLOCK
    positions = jnp.arange(SEQ_LEN)
    pos_weight = jnp.broadcast_to((positions < SEQ_LEN - 2).astype(jnp.float32), (BATCH_ROWS, SEQ_LEN))
    next_ids = jnp.roll(tokens, -1, axis=1)
    label_ids = jnp.roll(tokens, -2, axis=1)
    vocab_range = jnp.arange(VOCAB_SIZE)
    block_inputs = (
        hidden.reshape(n_blocks, ROW_BLOCK, MODEL_DIM),
        next_ids.reshape(n_blocks, ROW_BLOCK),
        label_ids.reshape(n_blocks, ROW_BLOCK),
        pos_weight.reshape(n_blocks, ROW_BLOCK),
    )

    def block_step(carry, block):
        d_out, d_emb, d_proj, d_gain_h, d_gain_e, d_gain_f, loss_sum = carry
        hid_blk, next_blk, label_blk, weight_blk = block
        hid_f32 = hid_blk.astype(jnp.float32)
        emb_f32 = jnp.take(emb_table, next_blk, axis=0).astype(jnp.float32)
        norm_h, vjp_h = jax.vjp(rms_norm, hid_f32, gain_h)
        norm_e, vjp_e = jax.vjp(rms_norm, emb_f32, gain_e)
        joined = jnp.concatenate([norm_h.astype(jnp.bfloat16), norm_e.astype(jnp.bfloat16)], axis=1)
        mixed = jnp.dot(joined, w_proj.T, preferred_element_type=jnp.float32)
        normed, vjp_f = jax.vjp(rms_norm, mixed, gain_f)
        features = normed.astype(jnp.bfloat16)
        logits = jnp.dot(features, out_table.T, preferred_element_type=jnp.float32)
        row_max = jnp.max(logits, axis=1, keepdims=True)
        log_norm = row_max[:, 0] + jnp.log(jnp.sum(jnp.exp(logits - row_max), axis=1))
        is_label = vocab_range[None, :] == label_blk[:, None]
        label_logit = jnp.sum(jnp.where(is_label, logits, 0.0), axis=1)
        loss_sum = loss_sum + jnp.sum(weight_blk * (log_norm - label_logit))
        soft_prob = jnp.exp(logits - log_norm[:, None])
        grad_logits = (MTP_WEIGHT * weight_blk[:, None] * (soft_prob - is_label.astype(jnp.float32))).astype(jnp.bfloat16)
        d_out = d_out + jnp.dot(grad_logits.T, features, preferred_element_type=jnp.float32)
        d_feats = jnp.dot(grad_logits, out_table, preferred_element_type=jnp.float32)
        d_mixed, grad_gf = vjp_f(d_feats)
        d_mixed_b = d_mixed.astype(jnp.bfloat16)
        d_proj = d_proj + jnp.dot(d_mixed_b.T, joined, preferred_element_type=jnp.float32)
        d_joined = jnp.dot(d_mixed_b, w_proj, preferred_element_type=jnp.float32)
        d_hid, grad_gh = vjp_h(d_joined[:, :MODEL_DIM])
        d_embrow, grad_ge = vjp_e(d_joined[:, MODEL_DIM:])
        d_emb = d_emb.at[next_blk].add(d_embrow)
        new_carry = (d_out, d_emb, d_proj, d_gain_h + grad_gh, d_gain_e + grad_ge, d_gain_f + grad_gf, loss_sum)
        return new_carry, d_hid.astype(jnp.bfloat16)

    init_carry = (
        jnp.zeros((VOCAB_SIZE, MODEL_DIM), jnp.float32),
        jnp.zeros((VOCAB_SIZE, MODEL_DIM), jnp.float32),
        jnp.zeros((MODEL_DIM, 2 * MODEL_DIM), jnp.float32),
        jnp.zeros((MODEL_DIM,), jnp.float32),
        jnp.zeros((MODEL_DIM,), jnp.float32),
        jnp.zeros((MODEL_DIM,), jnp.float32),
        jnp.zeros((), jnp.float32),
    )
    final_carry, d_hid_blocks = lax.scan(block_step, init_carry, block_inputs)
    d_out, d_emb, d_proj, d_gain_h, d_gain_e, d_gain_f, loss_sum = final_carry
    loss = (MTP_WEIGHT * loss_sum / (BATCH_ROWS * (SEQ_LEN - 2))).reshape(1)
    d_hidden = d_hid_blocks.reshape(BATCH_ROWS, SEQ_LEN, MODEL_DIM)
    return (loss, d_hidden, d_proj, d_emb, d_out, d_gain_h, d_gain_e, d_gain_f)
```

```python
import functools

import jax
import jax.numpy as jnp
from jax import lax
from jax.experimental import pallas as pl
from jax.experimental.pallas import tpu as pltpu
from jax.sharding import PartitionSpec as P

MTP_WEIGHT = 0.3
NORM_EPS = 1e-6
CORES = 2
LANES = 128
SUBLANES = 8
GROUP = 8
MESH = pl.DeviceIdType.MESH


def rms_norm(values, gain):
    scale = lax.rsqrt(jnp.mean(values * values, axis=-1, keepdims=True) + NORM_EPS)
    return values * scale * gain


def gather_kernel(nx, ny, de_ref, dh_ref, de_all, dh_all, de_own, dh_own, own_sem, send_sem, pair_send, recv_sem, pair_recv, dh_send, dh_recv):
    y = lax.axis_index("tp")
    cp = lax.axis_index("cp")
    x = cp // CORES
    c = cp % CORES
    xr, xl = (x + 1) % nx, (x + nx - 1) % nx
    yr, yl = (y + 1) % ny, (y + ny - 1) % ny

    def at(xx, cc, yy):
        return {"tp": yy, "cp": xx * CORES + cc}

    peers = [at(xr, c, y), at(xl, c, y), at(x, c, yr), at(x, c, yl), at(x, 1 - c, y)]
    barrier = pltpu.get_barrier_semaphore()
    for peer in peers:
        pl.semaphore_signal(barrier, inc=1, device_id=peer, device_id_type=MESH)
    pl.semaphore_wait(barrier, len(peers))

    half = de_ref.shape[0] // 2
    dh_half = dh_ref.shape[0] // 2
    started = []

    def push(src, dst, ssem, rsem, peer):
        copy = pltpu.make_async_remote_copy(src_ref=src, dst_ref=dst, send_sem=ssem, recv_sem=rsem, device_id=peer, device_id_type=MESH)
        copy.start()
        started.append(copy)

    def slot(yy, xx, cc, part=None):
        ref = de_all.at[yy, xx, cc]
        return ref if part is None else ref.at[pl.ds(part * half, half)]

    n_sends = [0]

    def send(src, yy, xx, part, peer):
        k = n_sends[0]
        n_sends[0] += 1
        push(src, slot(yy, xx, c, part), send_sem.at[k], recv_sem.at[yy, xx, part or 0], peer)

    def to_pair(src, yy, xx):
        push(src, slot(yy, xx, c), pair_send.at[yy, xx], pair_recv.at[yy, xx], at(x, 1 - c, y))

    def arrived(yy, xx, part=None):
        ref = slot(yy, xx, c, part)
        pltpu.make_async_copy(ref, ref, recv_sem.at[yy, xx, part or 0]).wait()

    n_dh = [0]

    def send_dh(src, yy, part, peer):
        k = n_dh[0]
        n_dh[0] += 1
        dst = dh_all.at[yy]
        if part is not None:
            dst = dst.at[pl.ds(part * dh_half, dh_half)]
        push(src, dst, dh_send.at[k], dh_recv.at[yy, part or 0], peer)

    def dh_arrived(yy, part=None):
        ref = dh_all.at[yy]
        if part is not None:
            ref = ref.at[pl.ds(part * dh_half, dh_half)]
        pltpu.make_async_copy(ref, ref, dh_recv.at[yy, part or 0]).wait()

    send(de_ref, y, x, None, at(xr, c, y))
    send(de_ref, y, x, None, at(xl, c, y))
    send(de_ref, y, x, None, at(x, c, yr))
    send(de_ref, y, x, None, at(x, c, yl))
    to_pair(de_ref, y, x)
    send_dh(dh_ref, y, None, at(x, c, yr))
    send_dh(dh_ref, y, None, at(x, c, yl))
    own_in = [pltpu.make_async_copy(de_ref, de_own, own_sem.at[0]), pltpu.make_async_copy(dh_ref, dh_own, own_sem.at[1])]
    for copy in own_in:
        copy.start()
    for copy in own_in:
        copy.wait()
    own_out = [pltpu.make_async_copy(de_own, slot(y, x, c), own_sem.at[0]), pltpu.make_async_copy(dh_own, dh_all.at[y], own_sem.at[1])]
    for copy in own_out:
        copy.start()

    def row_block(xx):
        send(slot(y, xx, c), y, xx, None, at(x, c, yr))
        send(slot(y, xx, c), y, xx, None, at(x, c, yl))
        to_pair(slot(y, xx, c), y, xx)

    order = [x]
    for dist in range(1, nx // 2):
        left, right = (x + nx - dist) % nx, (x + dist) % nx
        last = dist + 1 == nx // 2
        arrived(y, left)
        part = 0 if last else None
        send(slot(y, left, c, part), y, left, part, at(xr, c, y))
        row_block(left)
        arrived(y, right)
        part = 1 if last else None
        send(slot(y, right, c, part), y, right, part, at(xl, c, y))
        row_block(right)
        order += [left, right]
    far = (x + nx // 2) % nx
    arrived(y, far, 0)
    arrived(y, far, 1)
    row_block(far)
    order.append(far)

    for dist in range(1, ny // 2):
        down, up = (y + ny - dist) % ny, (y + dist) % ny
        last = dist + 1 == ny // 2
        for k, xx in enumerate(order):
            arrived(down, xx)
            part = 0 if last else None
            send(slot(down, xx, c, part), down, xx, part, at(x, c, yr))
            to_pair(slot(down, xx, c), down, xx)
            arrived(up, xx)
            part = 1 if last else None
            send(slot(up, xx, c, part), up, xx, part, at(x, c, yl))
            to_pair(slot(up, xx, c), up, xx)
            if k == 0:
                for yy, part, peer in ((down, 0, yr), (up, 1, yl)):
                    part = part if last else None
                    dh_arrived(yy)
                    src = dh_all.at[yy] if part is None else dh_all.at[yy].at[pl.ds(part * dh_half, dh_half)]
                    send_dh(src, yy, part, at(x, c, peer))
    far_y = (y + ny // 2) % ny
    for xx in order:
        arrived(far_y, xx, 0)
        arrived(far_y, xx, 1)
        to_pair(slot(far_y, xx, c), far_y, xx)
    dh_arrived(far_y, 0)
    dh_arrived(far_y, 1)
    for yy in range(ny):
        for xx in range(nx):
            ref = slot(yy, xx, 1 - c)
            pltpu.make_async_copy(ref, ref, pair_recv.at[yy, xx]).wait()
    for copy in own_out:
        copy.wait()
    for copy in started:
        copy.wait_send()


def gather_rows(mesh, de_tiles, dh_rows):
    ny, nx = mesh.shape["tp"], mesh.shape["cp"] // CORES
    hbm = pl.BlockSpec(memory_space=pl.ANY)
    n_sends = 2 + 2 + 2 * (nx // 2 - 1) + 2 * (nx - 1) + 2 * nx * (ny // 2 - 1)
    n_dh = 2 + 2 * (ny // 2 - 1)
    dma = pltpu.SemaphoreType.DMA
    moved = 4 * ((nx * ny * CORES) * de_tiles.size + ny * dh_rows.size)
    return pl.pallas_call(
        functools.partial(gather_kernel, nx, ny),
        out_shape=(
            jax.ShapeDtypeStruct((ny, nx, CORES) + de_tiles.shape, jnp.float32),
            jax.ShapeDtypeStruct((ny,) + dh_rows.shape, jnp.float32),
        ),
        in_specs=[hbm, hbm],
        out_specs=(hbm, hbm),
        scratch_shapes=[
            pltpu.VMEM(de_tiles.shape, jnp.float32),
            pltpu.VMEM(dh_rows.shape, jnp.float32),
            dma((2,)),
            dma((n_sends,)),
            dma((ny, nx)),
            dma((ny, nx, 2)),
            dma((ny, nx)),
            dma((n_dh,)),
            dma((ny, 2)),
        ],
        compiler_params=pltpu.CompilerParams(collective_id=0, has_side_effects=True),
        cost_estimate=pl.CostEstimate(flops=400_000_000_000, bytes_accessed=moved, transcendentals=0),
        name="gather_rows",
    )(de_tiles, dh_rows)


def scatter_kernel(row_ref, dup_ref, de_ref, out_ref, acc, sem, *, chunk, lanes):
    step = pl.program_id(0)
    zero_rows = 4 * SUBLANES * lanes

    @pl.when(step == 0)
    def _():
        def zero(i, carry):
            acc[pl.ds(pl.multiple_of(i * zero_rows, SUBLANES), zero_rows), :] = jnp.zeros((zero_rows, LANES), jnp.float32)
            return carry

        lax.fori_loop(0, acc.shape[0] // zero_rows, zero, 0)

    def group(k, carry):
        first = step * chunk + k * GROUP
        source = k * (lanes * SUBLANES)
        shared = dup_ref[step * (chunk // GROUP) + k]

        @pl.when(shared == 0)
        def _():
            rows = [row_ref[first + m] for m in range(GROUP)]
            sums = [acc[pl.ds(rows[m], lanes, stride=SUBLANES), :] + de_ref[pl.ds(source + m, lanes, stride=SUBLANES), :] for m in range(GROUP)]
            for m in range(GROUP):
                acc[pl.ds(rows[m], lanes, stride=SUBLANES), :] = sums[m]

        @pl.when(shared != 0)
        def _():
            for m in range(GROUP):
                here = pl.ds(row_ref[first + m], lanes, stride=SUBLANES)
                acc[here, :] = acc[here, :] + de_ref[pl.ds(source + m, lanes, stride=SUBLANES), :]

        return carry

    lax.fori_loop(0, chunk // GROUP, group, 0)

    @pl.when(step == pl.num_programs(0) - 1)
    def _():
        copy = pltpu.make_async_copy(acc.at[pl.ds(0, out_ref.shape[0])], out_ref, sem.at[0])
        copy.start()
        copy.wait()


def scatter_rows(local_ids, valid, de_tiles, vocab_blk, width, chunk):
    lanes = width // LANES
    n = local_ids.shape[0]
    tiles = vocab_blk // SUBLANES
    place = jnp.arange(n, dtype=jnp.int32)
    spare = tiles * SUBLANES * lanes + place % SUBLANES
    rows = jnp.where(valid, (local_ids // SUBLANES) * (SUBLANES * lanes) + local_ids % SUBLANES, spare)
    grouped = rows.reshape(n // GROUP, GROUP)
    shared = jnp.zeros((n // GROUP,), jnp.bool_)
    for s in range(1, GROUP):
        shared = shared | jnp.any(grouped[:, s:] == grouped[:, : GROUP - s], axis=1)
    acc_tiles = -(-(tiles + 1) // 4) * 4
    out = pl.pallas_call(
        functools.partial(scatter_kernel, chunk=chunk, lanes=lanes),
        out_shape=jax.ShapeDtypeStruct((tiles * lanes * SUBLANES, LANES), jnp.float32),
        grid_spec=pltpu.PrefetchScalarGridSpec(
            num_scalar_prefetch=2,
            grid=(n // chunk,),
            in_specs=[pl.BlockSpec((chunk * lanes, LANES), lambda i, *_: (i, 0))],
            out_specs=pl.BlockSpec(memory_space=pl.ANY),
            scratch_shapes=[pltpu.VMEM((acc_tiles * SUBLANES * lanes, LANES), jnp.float32), pltpu.SemaphoreType.DMA((1,))],
        ),
        compiler_params=pltpu.CompilerParams(vmem_limit_bytes=60 * 1024 * 1024),
        cost_estimate=pl.CostEstimate(flops=100_000_000_000, bytes_accessed=4 * (n + vocab_blk) * width, transcendentals=0),
        name="scatter_rows",
    )(rows, shared.astype(jnp.int32), de_tiles)
    return out.reshape(tiles, lanes, SUBLANES, LANES).transpose(0, 2, 1, 3).reshape(vocab_blk, width)


def solution(mesh):
    cp_size = mesh.shape["cp"]
    tp_size = mesh.shape["tp"]
    shift_pairs = [(src + 1, src) for src in range(cp_size - 1)]

    def local_step(hidden, tokens, emb_blk, out_blk, w_proj, gain_h, gain_e, gain_f):
        batch, piece_len, width = hidden.shape
        vocab_blk = emb_blk.shape[0]
        lanes = width // LANES
        share = batch // tp_size
        tp_rank = lax.axis_index("tp")
        cp_rank = lax.axis_index("cp")
        seq_len = piece_len * cp_size
        next_head = lax.ppermute(tokens[:, :2], "cp", shift_pairs)
        ext_ids = jnp.concatenate([tokens, next_head], axis=1)
        next_ids = ext_ids[:, 1 : piece_len + 1]
        label_ids = ext_ids[:, 2:]
        positions = cp_rank * piece_len + jnp.arange(piece_len)
        pos_weight = (positions < seq_len - 2).astype(jnp.float32)
        local_next = next_ids - tp_rank * vocab_blk
        in_block = (local_next >= 0) & (local_next < vocab_blk)
        emb_rows = jnp.take(emb_blk, jnp.clip(local_next, 0, vocab_blk - 1), axis=0).astype(jnp.float32)
        emb_rows = jnp.where(in_block[..., None], emb_rows, 0.0)
        emb_full = lax.psum(emb_rows, "tp")
        all_next = lax.all_gather(next_ids, "cp")
        all_next = all_next.reshape(cp_size, tp_size, share * piece_len).transpose(1, 0, 2).reshape(-1)

        def front(hid, emb):
            joined = jnp.concatenate([rms_norm(hid, gain_h).astype(jnp.bfloat16), rms_norm(emb, gain_e).astype(jnp.bfloat16)], axis=-1)
            return joined, jnp.einsum("bsk,nk->bsn", joined, w_proj, preferred_element_type=jnp.float32)

        joined, mixed = front(hidden.astype(jnp.float32), emb_full)
        features = rms_norm(mixed, gain_f).astype(jnp.bfloat16)
        logits = jnp.einsum("bsd,vd->bsv", features, out_blk, preferred_element_type=jnp.float32)
        part_max = jnp.max(logits, axis=-1)
        local_label = label_ids - tp_rank * vocab_blk
        is_label = jnp.arange(vocab_blk) == local_label[..., None]
        part_sum = jnp.sum(jnp.exp(logits - part_max[..., None]), axis=-1)
        part_label = jnp.sum(jnp.where(is_label, logits, 0.0), axis=-1)
        stats = lax.all_gather(jnp.stack([part_max, part_sum, part_label]), "tp")
        row_max = jnp.max(stats[:, 0], axis=0)
        exp_sum = jnp.sum(stats[:, 1] * jnp.exp(stats[:, 0] - row_max), axis=0)
        label_logit = jnp.sum(stats[:, 2], axis=0)
        log_norm = row_max + jnp.log(exp_sum)
        loss_part = jnp.where(tp_rank == 0, jnp.sum(pos_weight * (log_norm - label_logit)), 0.0)
        soft_prob = jnp.exp(logits - log_norm[..., None])
        grad_logits = (MTP_WEIGHT * pos_weight[:, None] * (soft_prob - is_label.astype(jnp.float32))).astype(jnp.bfloat16)
        d_feats = jnp.einsum("bsv,vd->bsd", grad_logits, out_blk, preferred_element_type=jnp.float32)
        d_feats = lax.psum_scatter(d_feats, "tp", scatter_dimension=0, tiled=True)
        d_out = jnp.einsum("bsv,bsd->vd", grad_logits, features, preferred_element_type=jnp.float32)
        d_out = lax.psum(d_out, "cp")

        def mine(value):
            return lax.dynamic_slice_in_dim(value, tp_rank * share, share, axis=0)

        hid_f32 = mine(hidden).astype(jnp.float32)
        _, vjp_h = jax.vjp(rms_norm, hid_f32, gain_h)
        _, vjp_e = jax.vjp(rms_norm, mine(emb_full), gain_e)
        _, vjp_f = jax.vjp(rms_norm, mine(mixed), gain_f)
        d_mixed, d_gain_f = vjp_f(d_feats)
        d_mixed_b = d_mixed.astype(jnp.bfloat16)
        d_proj = jnp.einsum("bsn,bsk->nk", d_mixed_b, mine(joined), preferred_element_type=jnp.float32)
        d_joined = jnp.einsum("bsn,nk->bsk", d_mixed_b, w_proj, preferred_element_type=jnp.float32)
        d_hid, d_gain_h = vjp_h(d_joined[..., :width])
        d_embrow, d_gain_e = vjp_e(d_joined[..., width:])

        rows = share * piece_len
        de_tiles = d_embrow.reshape(rows // SUBLANES, SUBLANES, lanes, LANES).transpose(0, 2, 1, 3).reshape(rows * lanes, LANES)
        de_all, dh_all = gather_rows(mesh, de_tiles, d_hid.reshape(rows, width))
        local_all = all_next - tp_rank * vocab_blk
        owned = (local_all >= 0) & (local_all < vocab_blk)
        d_emb = scatter_rows(local_all, owned, de_all.reshape(-1, LANES), vocab_blk, width, rows)
        d_hidden = dh_all.reshape(batch, piece_len, width).astype(jnp.bfloat16)

        last = jnp.concatenate([d_gain_f, loss_part.reshape(1), jnp.zeros((width - 1,), jnp.float32)])
        packed = jnp.concatenate([d_proj, jnp.concatenate([d_gain_h, d_gain_e])[None], last[None], jnp.zeros((SUBLANES - 2, 2 * width), jnp.float32)])
        packed = lax.psum(packed, ("tp", "cp"))
        d_proj = packed[:width]
        d_gain_h, d_gain_e = packed[width, :width], packed[width, width:]
        d_gain_f, loss_sum = packed[width + 1, :width], packed[width + 1, width]
        loss = (MTP_WEIGHT * loss_sum / (batch * (seq_len - 2))).reshape(1)
        return loss, d_hidden, d_proj, d_emb, d_out, d_gain_h, d_gain_e, d_gain_f

    part_seq = P("dp", "cp", None)
    in_specs = (part_seq, P("dp", "cp"), P("tp", None), P("tp", None), P(None, None), P(None), P(None), P(None))
    out_specs = (P("dp"), part_seq, P("dp", None), P(("dp", "tp"), None), P(("dp", "tp"), None), P("dp"), P("dp"), P("dp"))
    return jax.shard_map(local_step, mesh=mesh, in_specs=in_specs, out_specs=out_specs, check_vma=False)
```
